256 devices in a mesh: row: 32 (over x, z), col: 8 (over y, core).
Axes of the slice: x: 4, y: 4, z: 8, core: 2. Of those that a mesh axis runs over, the one named last changes fastest.
Arguments:
- features: bfloat16 [32768, 512], P(('row', 'col')), may hold values from -6 to 6
- adjacency: bfloat16 [32768, 32768], P('row', 'col'), may hold values from -0.19334951 to 0.19334951
- block_pattern: int32 [512, 512], P('row', 'col'), may hold values from 0 to 1, as said below
- weight_in: bfloat16 [512, 256], replicated, may hold values from -0.25 to 0.25
- bias_in: float32 [256], replicated, may hold values from -3 to 3
- weight_out: bfloat16 [256, 256], replicated, may hold values from -0.75 to 0.75
- bias_out: float32 [256], replicated, may hold values from -3 to 3
Outputs:
- embeddings: bfloat16 [32768, 256], P(('row', 'col'))
The draws below stay inside these ranges and needn't reach their ends.
Inputs may be any that keep to these rules, and one draw needn't show every extreme that they name: `block_pattern`: in each aligned tile of 16 rows by 64 columns, at most half of the entries are 1; some tile has exactly half.
All inputs are finite; a program needn't handle non-finite values.
Results may differ from the reference program's by a relative error of at most 0.015.
Values may be sent and summed in bfloat16 or wider, within the bound.
No kernel may reach another device: no remote copies, remote signals or barrier semaphores. Data moves between devices by JAX's collectives and lax.ppermute only.
A program may use at most 64 MiB of HBM per device.

```python
import math
import jax
import jax.numpy as jnp
from jax import lax

FIN = 512
HID = 256
BLK = 64
NODE_DEV = 128
NODES = 32768
TILE_ROWS = 1024
N_ROW = 32
N_COL = 8


def draw_adjacency(key, part):
    node_count = NODE_DEV * N_ROW * N_COL
    first_key, second_key, third_key = jax.random.split(jax.random.fold_in(key, 23), 3)
    values = jax.random.truncated_normal(first_key, -4.0, 4.0, (node_count, node_count), jnp.float32)
    row_scale = jnp.exp(0.5 * jax.random.uniform(second_key, (node_count, 1), jnp.float32, 0.0, math.log(10.0)))
    col_scale = jnp.exp(0.5 * jax.random.uniform(third_key, (1, node_count), jnp.float32, 0.0, math.log(10.0)))
    column_device = (jnp.arange(node_count, dtype=jnp.int32) // (NODE_DEV * N_ROW)).astype(jnp.float32)
    col_ramp = jnp.exp(0.5 * math.log(3.0) * column_device / max(N_COL - 1, 1))
    scaled_values = values * row_scale * col_scale * col_ramp[None, :] * (0.5 / math.sqrt(node_count))
    return scaled_values.astype(jnp.bfloat16)


def draw_block_pattern(key, part):
    row_blocks = NODE_DEV * N_COL // BLK
    col_blocks = NODE_DEV * N_ROW // BLK
    per_tile = row_blocks * col_blocks
    most_blocks = per_tile // 2
    tile_count = N_ROW * N_COL
    first_key, second_key, third_key = jax.random.split(jax.random.fold_in(key, 11), 3)
    spread = jax.random.randint(first_key, (tile_count,), 0, most_blocks + 1)
    counts = jnp.maximum(jnp.maximum(1, most_blocks // 8), spread * spread // max(most_blocks, 1))
    chosen = jax.random.randint(second_key, (), 0, tile_count)
    counts = jnp.where(jnp.arange(tile_count, dtype=jnp.int32) == chosen, most_blocks, counts)
    scores = jax.random.randint(third_key, (tile_count, per_tile), 0, (1 << 30) // per_tile)
    scores = scores * per_tile + jnp.arange(per_tile, dtype=jnp.int32)[None, :]
    rank_of = jnp.argsort(jnp.argsort(scores, axis=1), axis=1)
    pattern = (rank_of < counts[:, None]).astype(jnp.int32)
    pattern = pattern.reshape(N_ROW, N_COL, row_blocks, col_blocks).transpose(0, 2, 1, 3)
    return pattern.reshape(N_ROW * row_blocks, N_COL * col_blocks)


def levels(key, extent, shards, least, largest):
    def one(position, shards_of):
        draws = jax.random.uniform(jax.random.fold_in(jax.random.fold_in(key, 6), position), (shards_of,), jnp.float32, least / len(shards), largest / len(shards))
        return jnp.repeat(jnp.exp(draws), extent[position] // shards_of).reshape((-1,) + (1,) * (len(extent) - position - 1))

    gain = one(*shards[0])
    for cut in shards[1:]:
        gain = gain * one(*cut)
    return gain


def normal_values(rng, dims, scale, bound, cuts=(), held_as=jnp.bfloat16):
    entries = jax.random.normal(rng, dims, jnp.float32) * scale
    if len(cuts) > 0:
        entries = levels(rng, dims, cuts, -0.22, 0.18) * entries
    return jnp.clip(entries, min=-bound, max=bound).astype(held_as)


def setup_inputs(seed: int = 0) -> dict:
    splits = jax.random.split(jax.random.key(seed), 8)
    return {
        "features": normal_values(splits[0], (NODES, FIN), 1.0, 6.0, ((0, 256),)),
        "adjacency": draw_adjacency(jax.random.fold_in(splits[7], 71), 0),
        "block_pattern": draw_block_pattern(jax.random.fold_in(splits[7], 71), 0),
        "weight_in": normal_values(splits[3], (FIN, HID), FIN ** -0.5, 0.25),
        "bias_in": normal_values(splits[4], (HID,), 0.5, 3.0, (), jnp.float32),
        "weight_out": normal_values(splits[5], (HID, HID), (HID // 4) ** -0.5, 0.75),
        "bias_out": normal_values(splits[6], (HID,), 0.5, 3.0, (), jnp.float32),
    }


def stored_order(values):
    feat_width = values.shape[1]
    grid = values.reshape(N_ROW, N_COL, NODE_DEV, feat_width)
    return grid.transpose(1, 0, 2, 3).reshape(NODES, feat_width)

def masked_rows(adjacency, block_pattern, block_index):
    adj_rows = lax.dynamic_slice_in_dim(adjacency, block_index * TILE_ROWS, TILE_ROWS, 0).astype(jnp.float32)
    block_marks = lax.dynamic_slice_in_dim(block_pattern, block_index * (TILE_ROWS // BLK), TILE_ROWS // BLK, 0)
    present = jnp.repeat(jnp.repeat((block_marks == 1).astype(jnp.float32), BLK, axis=0), BLK, axis=1)
    return adj_rows * present

def aggregate(adjacency, block_pattern, scaled):
    source = stored_order(scaled).astype(jnp.float32)

    def one_block(block_index):
        return jnp.dot(masked_rows(adjacency, block_pattern, block_index), source, precision=lax.Precision.HIGHEST)
    return lax.map(one_block, jnp.arange(N_ROW, dtype=jnp.int32)).reshape(NODES, scaled.shape[1])

def reference(features, adjacency, block_pattern, weight_in, bias_in, weight_out, bias_out):

    def block_squares(block_index):
        return lax.optimization_barrier(jnp.sum(jnp.square(masked_rows(adjacency, block_pattern, block_index)), axis=1))
    squares = lax.map(block_squares, jnp.arange(N_ROW, dtype=jnp.int32)).reshape(NODES)
    inv_root = lax.rsqrt(1.0 + squares)[:, None]
    projected = jnp.dot(features, weight_in, preferred_element_type=jnp.float32)
    scaled = (inv_root * projected).astype(jnp.bfloat16)
    summed = aggregate(adjacency, block_pattern, scaled) + scaled.astype(jnp.float32)
    hidden = jax.nn.relu(inv_root * summed + bias_in[None, :]).astype(jnp.bfloat16)
    projected_out = jnp.dot(hidden, weight_out, preferred_element_type=jnp.float32)
    scaled_out = (inv_root * projected_out).astype(jnp.bfloat16)
    summed_out = aggregate(adjacency, block_pattern, scaled_out) + scaled_out.astype(jnp.float32)
    return (inv_root * summed_out + bias_out[None, :]).astype(jnp.bfloat16)
```

```python
import jax
import jax.numpy as jnp
from jax import lax
from jax.experimental import pallas as pl
from jax.experimental.pallas import tpu as pltpu
from jax.sharding import PartitionSpec as P

BLK = 64
NX = 4
NZ = 8
NY = 4
NROW = NX * NZ


def moved(offset, step):
    return ((offset[0] + step[0]) % NX, (offset[1] + step[1]) % NZ)


def row_shift(value, step):
    pairs = []
    for x in range(NX):
        for z in range(NZ):
            to = moved((x, z), step)
            pairs.append((x * NZ + z, to[0] * NZ + to[1]))
    return lax.ppermute(value, "row", pairs)


FAR = ((0, 0), (2, 2), (0, 4), (2, 6))
NEAR = ((1, 0), (3, 0), (0, 1), (0, 7))


def plan():
    first = list(FAR)
    for step in NEAR:
        first += [moved(o, step) for o in FAR]
    missing = [(x, z) for x in range(NX) for z in range(NZ) if (x, z) not in first]
    share = -(-len(missing) // len(NEAR))
    sends = [[] for _ in NEAR]

    def place(i):
        if i == len(missing):
            return True
        for n, step in enumerate(NEAR):
            source = moved(missing[i], (-step[0], -step[1]))
            if len(sends[n]) < share and source in first:
                sends[n].append(source)
                if place(i + 1):
                    return True
                sends[n].pop()
        return False

    assert place(0)
    for chosen in sends:
        chosen.sort(key=first.index)
    last = [moved(o, step) for step, chosen in zip(NEAR, sends) for o in chosen]
    return first, last, [[first.index(o) for o in chosen] for chosen in sends]


FIRST, LAST, SENDS = plan()
ORDER = FIRST + LAST


def picked(pieces, chosen, owned):
    per = pieces[0].shape[0] // owned
    runs = []
    for block in chosen:
        piece, at = divmod(block, per)
        if runs and runs[-1][0] == piece and runs[-1][2] == at:
            runs[-1][2] = at + 1
        else:
            runs.append([piece, at, at + 1])
    return jnp.concatenate([pieces[p][a * owned : b * owned] for p, a, b in runs])


def mask_kernel(row, pattern, adj, masked, squares, marks):
    step = pl.program_id(0)
    owned, width = adj.shape
    blocks = owned // BLK
    x, z = row[0] // NZ, row[0] % NZ
    source = [((x - dx) % NX) * NZ + (z - dz) % NZ for dx, dz in ORDER]

    @pl.when(step == 0)
    def _():
        pat = (pattern[...] == 1).astype(jnp.bfloat16)
        shape = (pat.shape[1], owned)
        block_of = lax.broadcasted_iota(jnp.int32, shape, 1) // BLK
        which = lax.broadcasted_iota(jnp.int32, shape, 0)
        for k in range(NROW):
            chosen = (which == block_of + source[k] * blocks).astype(jnp.bfloat16)
            spread = jnp.dot(pat, chosen, preferred_element_type=jnp.float32)
            for s in range(marks.shape[0]):
                marks[s, :, k * owned : (k + 1) * owned] = spread[s * blocks : (s + 1) * blocks]

    totals = [jnp.zeros((BLK, owned), jnp.float32) for _ in range(blocks)]
    for k in range(NROW):
        at = pl.multiple_of(source[k] * owned, owned)
        for b in range(blocks):
            mark = jnp.broadcast_to(marks[step, b : b + 1, k * owned : (k + 1) * owned], (BLK, owned))
            values = adj[b * BLK : (b + 1) * BLK, pl.ds(at, owned)] * mark.astype(jnp.bfloat16)
            masked[b * BLK : (b + 1) * BLK, k * owned : (k + 1) * owned] = values
            wide = values.astype(jnp.float32)
            totals[b] = totals[b] + wide * wide
    sums = lax.dot_general(
        jnp.ones((8, owned), jnp.float32),
        jnp.concatenate(totals),
        (((1,), (1,)), ((), ())),
        precision=lax.Precision.HIGHEST,
        preferred_element_type=jnp.float32,
    )
    squares[...] = sums[:1][None]


def masked_and_squares(row, pattern, adj):
    height, width = adj.shape
    owned = width // NROW
    steps = height // owned
    return pl.pallas_call(
        mask_kernel,
        out_shape=(
            jax.ShapeDtypeStruct(adj.shape, jnp.bfloat16),
            jax.ShapeDtypeStruct((steps, 1, owned), jnp.float32),
        ),
        grid_spec=pltpu.PrefetchScalarGridSpec(
            num_scalar_prefetch=1,
            grid=(steps,),
            in_specs=[
                pl.BlockSpec(pattern.shape, lambda i, row: (0, 0)),
                pl.BlockSpec((owned, width), lambda i, row: (i, 0)),
            ],
            out_specs=[
                pl.BlockSpec((owned, width), lambda i, row: (i, 0)),
                pl.BlockSpec((1, 1, owned), lambda i, row: (i, 0, 0)),
            ],
            scratch_shapes=[pltpu.VMEM((steps, owned // BLK, width), jnp.float32)],
        ),
        compiler_params=pltpu.CompilerParams(vmem_limit_bytes=16 * 2**20),
        name="mask_squares",
    )(row, pattern, pltpu.with_memory_space_constraint(adj, pltpu.HBM))


def first_kernel(masked, *refs):
    pieces, acc = refs[:-1], refs[-1]
    at = 0
    for i, piece in enumerate(pieces):
        end = at + piece.shape[0]
        part = jnp.dot(masked[:, at:end], piece[...], preferred_element_type=jnp.float32)
        acc[...] = part if i == 0 else acc[...] + part
        at = end


def last_kernel(place, masked, before, *refs):
    pieces, (keep, send) = refs[:-2], refs[-2:]
    width = sum(p.shape[0] for p in pieces)
    at = masked.shape[1] - width
    total = before[...]
    for piece in pieces:
        end = at + piece.shape[0]
        total = total + jnp.dot(masked[:, at:end], piece[...], preferred_element_type=jnp.float32)
        at = end
    owned = keep.shape[1]
    y, core = place[0] // 2, place[0] % 2
    for c in range(2 * NY):
        block = total[c * owned : (c + 1) * owned]
        slot = (c // 2 - y) % NY

        @pl.when(core == c % 2)
        def _():
            keep[slot] = block

        @pl.when(core != c % 2)
        def _():
            send[slot] = block.astype(send.dtype)


def in_vmem(count):
    return [pl.BlockSpec(memory_space=pltpu.VMEM)] * count


def product_first(masked, pieces):
    return pl.pallas_call(
        first_kernel,
        out_shape=jax.ShapeDtypeStruct((masked.shape[0], pieces[0].shape[1]), jnp.float32),
        in_specs=in_vmem(1 + len(pieces)),
        out_specs=pl.BlockSpec(memory_space=pltpu.VMEM),
        compiler_params=pltpu.CompilerParams(vmem_limit_bytes=16 * 2**20),
        name="product_first",
    )(masked, *pieces)


def product_last(place, masked, before, pieces):
    owned = masked.shape[0] // (2 * NY)
    shape = (NY, owned, pieces[0].shape[1])
    return pl.pallas_call(
        last_kernel,
        out_shape=(jax.ShapeDtypeStruct(shape, jnp.float32), jax.ShapeDtypeStruct(shape, jnp.bfloat16)),
        in_specs=[pl.BlockSpec(memory_space=pltpu.SMEM)] + in_vmem(2 + len(pieces)),
        out_specs=in_vmem(2),
        compiler_params=pltpu.CompilerParams(vmem_limit_bytes=16 * 2**20),
        name="product_last",
    )(place, masked, before, *pieces)


def aggregate(place, masked, own):
    owned = own.shape[0]
    column = jnp.concatenate([own] + [row_shift(own, step) for step in FAR[1:]])
    pieces = [column] + [row_shift(column, step) for step in NEAR]
    last = [row_shift(picked(pieces, chosen, owned), step) for step, chosen in zip(NEAR, SENDS)]
    keep, send = product_last(place, masked, product_first(masked, pieces), last)
    pair = keep + lax.ppermute(send, "col", [(i, i ^ 1) for i in range(2 * NY)]).astype(jnp.float32)
    total = pair[0]
    for s in (2, 1, 3):
        pairs = [(2 * y + k, 2 * ((y + s) % NY) + k) for y in range(NY) for k in range(2)]
        total = total + lax.ppermute(pair[s].astype(jnp.bfloat16), "col", pairs).astype(jnp.float32)
    return total + own.astype(jnp.float32)


def body(features, adjacency, block_pattern, weight_in, bias_in, weight_out, bias_out):
    row = lax.axis_index("row").astype(jnp.int32).reshape(1)
    place = lax.axis_index("col").astype(jnp.int32).reshape(1)
    masked, squares = masked_and_squares(row, block_pattern, adjacency)
    squares = lax.all_to_all(squares, "col", 0, 0, tiled=True)
    degree = 1.0 + jnp.sum(squares, axis=(0, 1))
    inv_root = lax.rsqrt(degree)[:, None]
    projected = jnp.dot(features, weight_in, preferred_element_type=jnp.float32)
    scaled = (inv_root * projected).astype(jnp.bfloat16)
    summed = aggregate(place, masked, scaled)
    hidden = jax.nn.relu(inv_root * summed + bias_in[None, :]).astype(jnp.bfloat16)
    scaled_out = (
        inv_root * jnp.dot(hidden, weight_out, preferred_element_type=jnp.float32)
    ).astype(jnp.bfloat16)
    summed_out = aggregate(place, masked, scaled_out)
    return (inv_root * summed_out + bias_out[None, :]).astype(jnp.bfloat16)


def solution(mesh):
    placed = (P(("row", "col"), None), P("row", "col"), P("row", "col"), P(), P(), P(), P())
    return jax.shard_map(
        body, mesh=mesh, in_specs=placed, out_specs=P(("row", "col"), None), check_vma=False
    )
```

```python
import functools

import jax
import jax.numpy as jnp
from jax import lax
from jax.experimental import pallas as pl
from jax.experimental.pallas import tpu as pltpu
from jax.sharding import PartitionSpec as P

BLK = 64
NX = 4
NZ = 8
NY = 4
NROW = NX * NZ


def moved(offset, step):
    return ((offset[0] + step[0]) % NX, (offset[1] + step[1]) % NZ)


def row_shift(value, step):
    pairs = []
    for x in range(NX):
        for z in range(NZ):
            to = moved((x, z), step)
            pairs.append((x * NZ + z, to[0] * NZ + to[1]))
    return lax.ppermute(value, "row", pairs)


FAR = ((0, 0), (2, 6), (0, 4), (2, 2))
NEAR = ((1, 0), (3, 0), (0, 1), (0, 7))
ONWARD = ((1, 0), (0, 1), (0, 7))
ORDER = list(FAR)
ORDER += [moved(o, step) for step in NEAR for o in FAR]
ORDER += [moved(moved(o, NEAR[0]), step) for step in ONWARD for o in FAR]
assert len(set(ORDER)) == NROW


def mask_kernel(device, pattern, adj, masked, squares, marks, marks_in, tiles, arrived, marks_arrived):
    steps, owned, width = tiles.shape
    blocks = owned // BLK
    x, z = device[0] // (2 * NY * NZ), device[0] // (2 * NY) % NZ
    source = [((x - dx) % NX) * NZ + (z - dz) % NZ for dx, dz in ORDER]

    def tile_copy(step):
        rows = pl.ds(pl.multiple_of(step * owned, owned), owned)
        return pltpu.make_async_copy(adj.at[rows, :], tiles.at[step], arrived.at[step])

    pattern_copy = pltpu.make_async_copy(pattern, marks_in, marks_arrived)
    pattern_copy.start()
    for step in range(steps):
        tile_copy(step).start()
    pattern_copy.wait()
    pat = (marks_in[...] == 1).astype(jnp.bfloat16)
    shape = (pat.shape[1], owned)
    block_of = lax.broadcasted_iota(jnp.int32, shape, 1) // BLK
    which = lax.broadcasted_iota(jnp.int32, shape, 0)
    for k in range(NROW):
        chosen = (which == block_of + source[k] * blocks).astype(jnp.bfloat16)
        spread = jnp.dot(pat, chosen, preferred_element_type=jnp.float32)
        for s in range(steps):
            marks[s, :, k * owned : (k + 1) * owned] = spread[s * blocks : (s + 1) * blocks]

    @pl.loop(0, steps)
    def _(step):
        tile_copy(step).wait()
        totals = [jnp.zeros((BLK, owned), jnp.float32) for _ in range(blocks)]
        for k in range(NROW):
            at = pl.multiple_of(source[k] * owned, owned)
            for b in range(blocks):
                mark = jnp.broadcast_to(marks[step, b : b + 1, k * owned : (k + 1) * owned], (16, owned))
                mark = mark.astype(jnp.bfloat16)[None]
                values = tiles[step, b * BLK : (b + 1) * BLK, pl.ds(at, owned)].reshape(-1, 16, owned) * mark
                values = values.reshape(BLK, owned)
                rows = pl.ds(pl.multiple_of(step * owned + b * BLK, BLK), BLK)
                masked[rows, k * owned : (k + 1) * owned] = values
                wide = values.astype(jnp.float32)
                totals[b] = totals[b] + wide * wide
        sums = lax.dot_general(
            jnp.ones((8, owned), jnp.float32),
            jnp.concatenate(totals),
            (((1,), (1,)), ((), ())),
            precision=lax.Precision.HIGHEST,
            preferred_element_type=jnp.float32,
        )
        squares[step] = sums[:1]


def masked_and_squares(device, pattern, adj):
    height, width = adj.shape
    owned = width // NROW
    steps = height // owned
    return pl.pallas_call(
        mask_kernel,
        out_shape=(
            pltpu.VMEM(adj.shape, jnp.bfloat16),
            jax.ShapeDtypeStruct((steps, 1, owned), jnp.float32),
        ),
        in_specs=[pl.BlockSpec(memory_space=pltpu.SMEM)] + [pl.BlockSpec(memory_space=pltpu.HBM)] * 2,
        out_specs=in_vmem(2),
        scratch_shapes=[
            pltpu.VMEM((steps, owned // BLK, width), jnp.float32),
            pltpu.VMEM(pattern.shape, pattern.dtype),
            pltpu.VMEM((steps, owned, width), adj.dtype),
            pltpu.SemaphoreType.DMA((steps,)),
            pltpu.SemaphoreType.DMA,
        ],
        compiler_params=pltpu.CompilerParams(vmem_limit_bytes=16 * 2**20),
        name="mask_squares",
    )(device, *(pltpu.with_memory_space_constraint(a, pltpu.HBM) for a in (pattern, adj)))


def first_kernel(masked, *refs):
    pieces, acc = refs[:-1], refs[-1]
    at = 0
    for i, piece in enumerate(pieces):
        end = at + piece.shape[0]
        part = jnp.dot(masked[:, at:end], piece[...], preferred_element_type=jnp.float32)
        acc[...] = part if i == 0 else acc[...] + part
        at = end


def last_kernel(sibling, device, masked, before, *refs):
    pieces, out = refs[:-1], refs[-1]
    width = sum(p.shape[0] for p in pieces)
    at = masked.shape[1] - width
    owned = out.shape[1]
    y, core = device[0] // 2 % NY, (device[0] + sibling) % 2
    rows = [pl.ds(pl.multiple_of((2 * ((y + s) % NY) + core) * owned, owned), owned) for s in range(NY)]
    total = jnp.concatenate([before[r, :] for r in rows])
    for piece in pieces:
        end = at + piece.shape[0]
        part = jnp.concatenate([masked[r, at:end] for r in rows])
        total = total + jnp.dot(part, piece[...], preferred_element_type=jnp.float32)
        at = end
    out[...] = total.reshape(out.shape).astype(out.dtype)


def in_vmem(count):
    return [pl.BlockSpec(memory_space=pltpu.VMEM)] * count


def product_first(masked, pieces):
    return pl.pallas_call(
        first_kernel,
        out_shape=jax.ShapeDtypeStruct((masked.shape[0], pieces[0].shape[1]), jnp.float32),
        in_specs=in_vmem(1 + len(pieces)),
        out_specs=pl.BlockSpec(memory_space=pltpu.VMEM),
        compiler_params=pltpu.CompilerParams(vmem_limit_bytes=16 * 2**20),
        name="product_first",
    )(masked, *pieces)


def product_last(device, masked, before, pieces, sibling):
    owned = masked.shape[0] // (2 * NY)
    shape = (NY, owned, pieces[0].shape[1])
    return pl.pallas_call(
        functools.partial(last_kernel, sibling),
        out_shape=jax.ShapeDtypeStruct(shape, jnp.bfloat16 if sibling else jnp.float32),
        in_specs=[pl.BlockSpec(memory_space=pltpu.SMEM)] + in_vmem(2 + len(pieces)),
        out_specs=pl.BlockSpec(memory_space=pltpu.VMEM),
        compiler_params=pltpu.CompilerParams(vmem_limit_bytes=16 * 2**20),
        name="product_send" if sibling else "product_keep",
    )(device, masked, before, *pieces)


def aggregate(device, masked, own):
    column = jnp.concatenate([own] + [row_shift(own, step) for step in FAR[1:]])
    near = [row_shift(column, step) for step in NEAR]
    onward = [row_shift(near[0], step) for step in ONWARD]
    before = product_first(masked, [column] + near)
    send = product_last(device, masked, before, onward, 1)
    send = lax.ppermute(send, "col", [(i, i ^ 1) for i in range(2 * NY)])
    pair = product_last(device, masked, before, onward, 0) + send.astype(jnp.float32)
    total = pair[0]
    for s in (2, 1, 3):
        pairs = [(2 * y + k, 2 * ((y + s) % NY) + k) for y in range(NY) for k in range(2)]
        total = total + lax.ppermute(pair[s].astype(jnp.bfloat16), "col", pairs).astype(jnp.float32)
    return total + own.astype(jnp.float32)


def body(features, adjacency, block_pattern, weight_in, bias_in, weight_out, bias_out):
    device = lax.axis_index(("row", "col")).astype(jnp.int32).reshape(1)
    masked, squares = masked_and_squares(device, block_pattern, adjacency)
    squares = lax.all_to_all(squares, "col", 0, 0, tiled=True)
    degree = jnp.ones_like(squares[0, 0])
    for part in range(squares.shape[0]):
        degree = degree + squares[part, 0]
    inv_root = lax.rsqrt(degree)[:, None]
    projected = jnp.dot(features, weight_in, preferred_element_type=jnp.float32)
    scaled = (inv_root * projected).astype(jnp.bfloat16)
    summed = aggregate(device, masked, scaled)
    hidden = jax.nn.relu(inv_root * summed + bias_in[None, :]).astype(jnp.bfloat16)
    scaled_out = (
        inv_root * jnp.dot(hidden, weight_out, preferred_element_type=jnp.float32)
    ).astype(jnp.bfloat16)
    summed_out = aggregate(device, masked, scaled_out)
    return (inv_root * summed_out + bias_out[None, :]).astype(jnp.bfloat16)


def solution(mesh):
    placed = (P(("row", "col"), None), P("row", "col"), P("row", "col"), P(), P(), P(), P())
    return jax.shard_map(
        body, mesh=mesh, in_specs=placed, out_specs=P(("row", "col"), None), check_vma=False
    )
```

```python
import functools

import jax
import jax.numpy as jnp
from jax import lax
from jax.experimental import pallas as pl
from jax.experimental.pallas import tpu as pltpu
from jax.sharding import PartitionSpec as P

BLK = 64
PACK = 16
LOADS = 2
NX = 4
NZ = 8
NY = 4
NROW = NX * NZ


def moved(offset, step):
    return ((offset[0] + step[0]) % NX, (offset[1] + step[1]) % NZ)


def row_shift(value, step):
    pairs = []
    for x in range(NX):
        for z in range(NZ):
            to = moved((x, z), step)
            pairs.append((x * NZ + z, to[0] * NZ + to[1]))
    return lax.ppermute(value, "row", pairs)


FAR = ((0, 0), (2, 6), (0, 4), (2, 2))
NEAR = ((1, 0), (3, 0), (0, 1), (0, 7))
ONWARD = ((1, 0), (0, 1), (0, 7))
ORDER = list(FAR)
ORDER += [moved(o, step) for step in NEAR for o in FAR]
ORDER += [moved(moved(o, NEAR[0]), step) for step in ONWARD for o in FAR]
assert len(set(ORDER)) == NROW


def squares_kernel(device, pattern, adj, tiles, squares, choose, marks, totals, arrived, marks_arrived):
    del device
    height, width = tiles.shape
    steps = arrived.shape[0]
    tall = height // steps
    owned = squares.shape[2]

    def tile_copy(step):
        rows = pl.ds(pl.multiple_of(step * tall, tall), tall)
        return pltpu.make_async_copy(adj.at[rows, :], tiles.at[rows, :], arrived.at[step])

    pattern_copy = pltpu.make_async_copy(pattern, marks, marks_arrived)
    pattern_copy.start()
    for step in range(steps):
        tile_copy(step).start()
    lanes = choose.shape[1]
    column = lax.broadcasted_iota(jnp.int32, (BLK, lanes), 1)
    for j in range(width // BLK):
        choose[j * BLK : (j + 1) * BLK, :] = (column == j).astype(choose.dtype)
    pattern_copy.wait()

    @pl.loop(0, steps)
    def _(step):
        tile_copy(step).wait()
        rows = pl.ds(pl.multiple_of(step * tall, tall), tall)
        values = tiles[rows, :]
        totals[rows, :] = jnp.dot(values * values, choose[...], preferred_element_type=jnp.float32)

    for c in range(squares.shape[0]):
        here = marks[c * owned // BLK : (c + 1) * owned // BLK, :]
        present = [jnp.broadcast_to(here[b : b + 1] == 1, (BLK, here.shape[1])) for b in range(owned // BLK)]
        sums = totals[c * owned : (c + 1) * owned, : here.shape[1]]
        sums = jnp.where(jnp.concatenate(present), sums, 0.0)
        sums = lax.dot_general(
            jnp.ones((8, sums.shape[1]), jnp.float32),
            sums,
            (((1,), (1,)), ((), ())),
            precision=lax.Precision.HIGHEST,
            preferred_element_type=jnp.float32,
        )
        squares[c] = sums[:1]


def spread_marks(pattern, marks, source, owned):
    pat = (pattern[...] == 1).astype(jnp.bfloat16)
    shape = (pat.shape[1], owned)
    block_of = lax.broadcasted_iota(jnp.int32, shape, 1) // BLK
    which = lax.broadcasted_iota(jnp.int32, shape, 0)
    for k in range(NROW):
        chosen = (which == block_of + source[k] * (owned // BLK)).astype(jnp.bfloat16)
        spread = jnp.dot(pat, chosen, preferred_element_type=jnp.float32)
        for b in range(spread.shape[0]):
            mark = jnp.broadcast_to(spread[b : b + 1], (PACK, owned)).astype(jnp.bfloat16)
            marks[b, :, k * owned : (k + 1) * owned] = mark


def mask_kernel(device, pattern, adj, after, masked, marks):
    del after
    height, width = adj.shape
    owned = width // NROW
    x, z = device[0] // (2 * NY * NZ), device[0] // (2 * NY) % NZ
    source = [((x - dx) % NX) * NZ + (z - dz) % NZ for dx, dz in ORDER]
    spread_marks(pattern, marks, source, owned)

    @pl.loop(0, height // BLK)
    def _(part):
        for k in range(NROW):
            here = slice(k * owned, (k + 1) * owned)
            at = pl.ds(pl.multiple_of(source[k] * owned, owned), owned)
            mark = marks[part, :, here]
            for r in range(BLK // PACK):
                rows = pl.ds(pl.multiple_of(part * BLK + r * PACK, PACK), PACK)
                masked[rows, here] = adj[rows, at] * mark


def loaded_and_squares(device, pattern, adj):
    height, width = adj.shape
    owned = width // NROW
    return pl.pallas_call(
        squares_kernel,
        out_shape=(
            pltpu.VMEM(adj.shape, adj.dtype),
            jax.ShapeDtypeStruct((height // owned, 1, owned), jnp.float32),
        ),
        in_specs=[pl.BlockSpec(memory_space=pltpu.SMEM)] + [pl.BlockSpec(memory_space=pltpu.HBM)] * 2,
        out_specs=in_vmem(2),
        scratch_shapes=[
            pltpu.VMEM((width, 128), jnp.bfloat16),
            pltpu.VMEM(pattern.shape, pattern.dtype),
            pltpu.VMEM((height, 128), jnp.float32),
            pltpu.SemaphoreType.DMA((LOADS,)),
            pltpu.SemaphoreType.DMA,
        ],
        compiler_params=pltpu.CompilerParams(vmem_limit_bytes=8 * 2**20),
        name="load_squares",
    )(device, *(pltpu.with_memory_space_constraint(a, pltpu.HBM) for a in (pattern, adj)))


def masked_in_order(device, pattern, adj, after):
    height, width = adj.shape
    return pl.pallas_call(
        mask_kernel,
        out_shape=pltpu.VMEM(adj.shape, adj.dtype),
        in_specs=[pl.BlockSpec(memory_space=pltpu.SMEM)] + in_vmem(3),
        out_specs=pl.BlockSpec(memory_space=pltpu.VMEM),
        scratch_shapes=[pltpu.VMEM((height // BLK, PACK, width), jnp.bfloat16)],
        compiler_params=pltpu.CompilerParams(vmem_limit_bytes=8 * 2**20),
        name="mask_in_order",
    )(device, pattern, adj, after)


def first_kernel(masked, *refs):
    pieces, acc = refs[:-1], refs[-1]
    at = 0
    for i, piece in enumerate(pieces):
        end = at + piece.shape[0]
        part = jnp.dot(masked[:, at:end], piece[...], preferred_element_type=jnp.float32)
        acc[...] = part if i == 0 else acc[...] + part
        at = end


def last_kernel(sibling, device, masked, before, *refs):
    pieces, out = refs[:-1], refs[-1]
    width = sum(p.shape[0] for p in pieces)
    at = masked.shape[1] - width
    owned = out.shape[1]
    y, core = device[0] // 2 % NY, (device[0] + sibling) % 2
    rows = [pl.ds(pl.multiple_of((2 * ((y + s) % NY) + core) * owned, owned), owned) for s in range(NY)]
    total = jnp.concatenate([before[r, :] for r in rows])
    for piece in pieces:
        end = at + piece.shape[0]
        part = jnp.concatenate([masked[r, at:end] for r in rows])
        total = total + jnp.dot(part, piece[...], preferred_element_type=jnp.float32)
        at = end
    out[...] = total.reshape(out.shape).astype(out.dtype)


def in_vmem(count):
    return [pl.BlockSpec(memory_space=pltpu.VMEM)] * count


def product_first(masked, pieces):
    return pl.pallas_call(
        first_kernel,
        out_shape=jax.ShapeDtypeStruct((masked.shape[0], pieces[0].shape[1]), jnp.float32),
        in_specs=in_vmem(1 + len(pieces)),
        out_specs=pl.BlockSpec(memory_space=pltpu.VMEM),
        compiler_params=pltpu.CompilerParams(vmem_limit_bytes=16 * 2**20),
        name="product_first",
    )(masked, *pieces)


def product_last(device, masked, before, pieces, sibling):
    owned = masked.shape[0] // (2 * NY)
    shape = (NY, owned, pieces[0].shape[1])
    return pl.pallas_call(
        functools.partial(last_kernel, sibling),
        out_shape=jax.ShapeDtypeStruct(shape, jnp.bfloat16 if sibling else jnp.float32),
        in_specs=[pl.BlockSpec(memory_space=pltpu.SMEM)] + in_vmem(2 + len(pieces)),
        out_specs=pl.BlockSpec(memory_space=pltpu.VMEM),
        compiler_params=pltpu.CompilerParams(vmem_limit_bytes=16 * 2**20),
        name="product_send" if sibling else "product_keep",
    )(device, masked, before, *pieces)


def aggregate(device, masked, own):
    column = jnp.concatenate([own] + [row_shift(own, step) for step in FAR[1:]])
    near = [row_shift(column, step) for step in NEAR]
    onward = [row_shift(near[0], step) for step in ONWARD]
    before = product_first(masked, [column] + near)
    send = product_last(device, masked, before, onward, 1)
    send = lax.ppermute(send, "col", [(i, i ^ 1) for i in range(2 * NY)])
    pair = product_last(device, masked, before, onward, 0) + send.astype(jnp.float32)
    total = pair[0]
    for s in (2, 1, 3):
        pairs = [(2 * y + k, 2 * ((y + s) % NY) + k) for y in range(NY) for k in range(2)]
        total = total + lax.ppermute(pair[s].astype(jnp.bfloat16), "col", pairs).astype(jnp.float32)
    return total + own.astype(jnp.float32)


def body(features, adjacency, block_pattern, weight_in, bias_in, weight_out, bias_out):
    device = lax.axis_index(("row", "col")).astype(jnp.int32).reshape(1)
    loaded, squares = loaded_and_squares(device, block_pattern, adjacency)
    squares = lax.all_to_all(squares, "col", 0, 0, tiled=True)
    degree = jnp.ones_like(squares[0, 0])
    for part in range(squares.shape[0]):
        degree = degree + squares[part, 0]
    inv_root = lax.rsqrt(degree)[:, None]
    projected = jnp.dot(features, weight_in, preferred_element_type=jnp.float32)
    scaled = (inv_root * projected).astype(jnp.bfloat16)
    masked = masked_in_order(device, block_pattern, loaded, scaled)
    summed = aggregate(device, masked, scaled)
    hidden = jax.nn.relu(inv_root * summed + bias_in[None, :]).astype(jnp.bfloat16)
    scaled_out = (
        inv_root * jnp.dot(hidden, weight_out, preferred_element_type=jnp.float32)
    ).astype(jnp.bfloat16)
    summed_out = aggregate(device, masked, scaled_out)
    return (inv_root * summed_out + bias_out[None, :]).astype(jnp.bfloat16)


def solution(mesh):
    placed = (P(("row", "col"), None), P("row", "col"), P("row", "col"), P(), P(), P(), P())
    return jax.shard_map(
        body, mesh=mesh, in_specs=placed, out_specs=P(("row", "col"), None), check_vma=False
    )
```

```python
import functools

import jax
import jax.numpy as jnp
from jax import lax
from jax.experimental import pallas as pl
from jax.experimental.pallas import tpu as pltpu
from jax.sharding import PartitionSpec as P

BLK = 64
PACK = 16
LOADS = 2
NX = 4
NZ = 8
NY = 4
NROW = NX * NZ


def moved(offset, step):
    return ((offset[0] + step[0]) % NX, (offset[1] + step[1]) % NZ)


def row_shift(value, step):
    pairs = []
    for x in range(NX):
        for z in range(NZ):
            to = moved((x, z), step)
            pairs.append((x * NZ + z, to[0] * NZ + to[1]))
    return lax.ppermute(value, "row", pairs)


FAR = ((0, 0), (2, 6), (0, 4), (2, 2))
NEAR = ((1, 0), (3, 0), (0, 1), (0, 7))
ONWARD = ((1, 0), (0, 1), (0, 7))
ORDER = list(FAR)
ORDER += [moved(o, step) for step in NEAR for o in FAR]
ORDER += [moved(moved(o, NEAR[0]), step) for step in ONWARD for o in FAR]
assert len(set(ORDER)) == NROW


def squares_kernel(device, pattern, adj, tiles, squares, choose, marks, totals, arrived, marks_arrived):
    del device
    height, width = tiles.shape
    steps = arrived.shape[0]
    tall = height // steps
    owned = squares.shape[2]

    def tile_copy(step):
        rows = pl.ds(pl.multiple_of(step * tall, tall), tall)
        return pltpu.make_async_copy(adj.at[rows, :], tiles.at[rows, :], arrived.at[step])

    pattern_copy = pltpu.make_async_copy(pattern, marks, marks_arrived)
    pattern_copy.start()
    for step in range(steps):
        tile_copy(step).start()
    lanes = choose.shape[1]
    column = lax.broadcasted_iota(jnp.int32, (BLK, lanes), 1)
    for j in range(width // BLK):
        choose[j * BLK : (j + 1) * BLK, :] = (column == j).astype(choose.dtype)
    pattern_copy.wait()

    @pl.loop(0, steps)
    def _(step):
        tile_copy(step).wait()
        rows = pl.ds(pl.multiple_of(step * tall, tall), tall)
        values = tiles[rows, :]
        totals[rows, :] = jnp.dot(values * values, choose[...], preferred_element_type=jnp.float32)

    for c in range(squares.shape[0]):
        here = marks[c * owned // BLK : (c + 1) * owned // BLK, :]
        present = [jnp.broadcast_to(here[b : b + 1] == 1, (BLK, here.shape[1])) for b in range(owned // BLK)]
        sums = totals[c * owned : (c + 1) * owned, : here.shape[1]]
        sums = jnp.where(jnp.concatenate(present), sums, 0.0)
        sums = lax.dot_general(
            jnp.ones((8, sums.shape[1]), jnp.float32),
            sums,
            (((1,), (1,)), ((), ())),
            precision=lax.Precision.HIGHEST,
            preferred_element_type=jnp.float32,
        )
        squares[c] = sums[:1]


def spread_marks(pattern, marks, source, owned):
    pat = (pattern[...] == 1).astype(jnp.bfloat16)
    shape = (pat.shape[1], owned)
    block_of = lax.broadcasted_iota(jnp.int32, shape, 1) // BLK
    which = lax.broadcasted_iota(jnp.int32, shape, 0)
    for k in range(NROW):
        chosen = (which == block_of + source[k] * (owned // BLK)).astype(jnp.bfloat16)
        spread = jnp.dot(pat, chosen, preferred_element_type=jnp.float32)
        for b in range(spread.shape[0]):
            mark = jnp.broadcast_to(spread[b : b + 1], (PACK, owned)).astype(jnp.bfloat16)
            marks[b, :, k * owned : (k + 1) * owned] = mark


def mask_kernel(device, pattern, adj, after, masked, marks):
    del after
    height, width = adj.shape
    owned = width // NROW
    x, z = device[0] // (2 * NY * NZ), device[0] // (2 * NY) % NZ
    source = [((x - dx) % NX) * NZ + (z - dz) % NZ for dx, dz in ORDER]
    spread_marks(pattern, marks, source, owned)

    @pl.loop(0, height // BLK)
    def _(part):
        for k in range(NROW):
            here = slice(k * owned, (k + 1) * owned)
            at = pl.ds(pl.multiple_of(source[k] * owned, owned), owned)
            mark = marks[part, :, here]
            for r in range(BLK // PACK):
                rows = pl.ds(pl.multiple_of(part * BLK + r * PACK, PACK), PACK)
                masked[rows, here] = adj[rows, at] * mark


def loaded_and_squares(device, pattern, adj):
    height, width = adj.shape
    owned = width // NROW
    return pl.pallas_call(
        squares_kernel,
        out_shape=(
            pltpu.VMEM(adj.shape, adj.dtype),
            jax.ShapeDtypeStruct((height // owned, 1, owned), jnp.float32),
        ),
        in_specs=[pl.BlockSpec(memory_space=pltpu.SMEM)] + [pl.BlockSpec(memory_space=pltpu.HBM)] * 2,
        out_specs=in_vmem(2),
        scratch_shapes=[
            pltpu.VMEM((width, 128), jnp.bfloat16),
            pltpu.VMEM(pattern.shape, pattern.dtype),
            pltpu.VMEM((height, 128), jnp.float32),
            pltpu.SemaphoreType.DMA((LOADS,)),
            pltpu.SemaphoreType.DMA,
        ],
        compiler_params=pltpu.CompilerParams(vmem_limit_bytes=8 * 2**20),
        name="load_squares",
    )(device, *(pltpu.with_memory_space_constraint(a, pltpu.HBM) for a in (pattern, adj)))


def masked_in_order(device, pattern, adj, after):
    height, width = adj.shape
    return pl.pallas_call(
        mask_kernel,
        out_shape=pltpu.VMEM(adj.shape, adj.dtype),
        in_specs=[pl.BlockSpec(memory_space=pltpu.SMEM)] + in_vmem(3),
        out_specs=pl.BlockSpec(memory_space=pltpu.VMEM),
        scratch_shapes=[pltpu.VMEM((height // BLK, PACK, width), jnp.bfloat16)],
        compiler_params=pltpu.CompilerParams(vmem_limit_bytes=8 * 2**20),
        name="mask_in_order",
    )(device, pattern, adj, after)


def first_kernel(masked, *refs):
    pieces, acc = refs[:-1], refs[-1]
    at = 0
    for i, piece in enumerate(pieces):
        end = at + piece.shape[0]
        part = jnp.dot(masked[:, at:end], piece[...], preferred_element_type=jnp.float32)
        acc[...] = part if i == 0 else acc[...] + part
        at = end


def last_kernel(sibling, device, masked, before, *refs):
    pieces, out = refs[:-1], refs[-1]
    width = sum(p.shape[0] for p in pieces)
    at = masked.shape[1] - width
    owned = out.shape[1]
    y, core = device[0] // 2 % NY, (device[0] + sibling) % 2
    rows = [pl.ds(pl.multiple_of((2 * ((y + s) % NY) + core) * owned, owned), owned) for s in range(NY)]
    total = jnp.concatenate([before[r, :] for r in rows])
    for piece in pieces:
        end = at + piece.shape[0]
        part = jnp.concatenate([masked[r, at:end] for r in rows])
        total = total + jnp.dot(part, piece[...], preferred_element_type=jnp.float32)
        at = end
    out[...] = total.reshape(out.shape).astype(out.dtype)


def in_vmem(count):
    return [pl.BlockSpec(memory_space=pltpu.VMEM)] * count


def product_first(masked, pieces):
    return pl.pallas_call(
        first_kernel,
        out_shape=jax.ShapeDtypeStruct((masked.shape[0], pieces[0].shape[1]), jnp.float32),
        in_specs=in_vmem(1 + len(pieces)),
        out_specs=pl.BlockSpec(memory_space=pltpu.VMEM),
        compiler_params=pltpu.CompilerParams(vmem_limit_bytes=16 * 2**20),
        name="product_first",
    )(masked, *pieces)


def product_last(device, masked, before, pieces, sibling):
    owned = masked.shape[0] // (2 * NY)
    shape = (NY, owned, pieces[0].shape[1])
    return pl.pallas_call(
        functools.partial(last_kernel, sibling),
        out_shape=jax.ShapeDtypeStruct(shape, jnp.bfloat16 if sibling else jnp.float32),
        in_specs=[pl.BlockSpec(memory_space=pltpu.SMEM)] + in_vmem(2 + len(pieces)),
        out_specs=pl.BlockSpec(memory_space=pltpu.VMEM),
        compiler_params=pltpu.CompilerParams(vmem_limit_bytes=16 * 2**20),
        name="product_send" if sibling else "product_keep",
    )(device, masked, before, *pieces)


def aggregate(device, masked, own):
    far, masked = lax.optimization_barrier(([row_shift(own, step) for step in FAR[1:]], masked))
    column = jnp.concatenate([own] + far)
    near = [row_shift(column, step) for step in NEAR]
    onward = [row_shift(near[0], step) for step in ONWARD]
    before = product_first(masked, [column] + near)
    send = product_last(device, masked, before, onward, 1)
    send = lax.ppermute(send, "col", [(i, i ^ 1) for i in range(2 * NY)])
    pair = product_last(device, masked, before, onward, 0) + send.astype(jnp.float32)
    total = pair[0]
    for s in (2, 1, 3):
        pairs = [(2 * y + k, 2 * ((y + s) % NY) + k) for y in range(NY) for k in range(2)]
        total = total + lax.ppermute(pair[s].astype(jnp.bfloat16), "col", pairs).astype(jnp.float32)
    return total + own.astype(jnp.float32)


def body(features, adjacency, block_pattern, weight_in, bias_in, weight_out, bias_out):
    device = lax.axis_index(("row", "col")).astype(jnp.int32).reshape(1)
    loaded, squares = loaded_and_squares(device, block_pattern, adjacency)
    squares = lax.all_to_all(squares, "col", 0, 0, tiled=True)
    degree = jnp.ones_like(squares[0, 0])
    for part in range(squares.shape[0]):
        degree = degree + squares[part, 0]
    inv_root = lax.rsqrt(degree)[:, None]
    projected = jnp.dot(features, weight_in, preferred_element_type=jnp.float32)
    scaled = (inv_root * projected).astype(jnp.bfloat16)
    masked = masked_in_order(device, block_pattern, loaded, scaled)
    summed = aggregate(device, masked, scaled)
    hidden = jax.nn.relu(inv_root * summed + bias_in[None, :]).astype(jnp.bfloat16)
    scaled_out = (
        inv_root * jnp.dot(hidden, weight_out, preferred_element_type=jnp.float32)
    ).astype(jnp.bfloat16)
    summed_out = aggregate(device, masked, scaled_out)
    return (inv_root * summed_out + bias_out[None, :]).astype(jnp.bfloat16)


def solution(mesh):
    placed = (P(("row", "col"), None), P("row", "col"), P("row", "col"), P(), P(), P(), P())
    return jax.shard_map(
        body, mesh=mesh, in_specs=placed, out_specs=P(("row", "col"), None), check_vma=False
    )
```
